32 devices in a mesh: section: 4 (over x, core), expert: 4 (over z), tensor: 2 (over y).
Axes of the slice: x: 2, y: 2, z: 4, core: 2. Of those that a mesh axis runs over, the one named last changes fastest.
Arguments:
- tokens: bfloat16 [2, 4, 512, 2048], P(None, 'section', ('expert', 'tensor')), may hold values from -26 to 26
- norm_gain: bfloat16 [4, 2048], P('section'), may hold values from 0.099609375 to 1.8984375
- router_weight: bfloat16 [4, 2048, 4], P('section'), may hold values from -0.125 to 0.125
- gate_up: bfloat16 [4, 4, 2048, 5632], P('section', 'expert', None, 'tensor'), may hold values from -0.125 to 0.125
- down_proj: bfloat16 [4, 4, 2816, 2048], P('section', 'expert', 'tensor'), may hold values from -0.109375 to 0.109375
- expert_ids: int32 [2, 2, 4, 512, 2], P(None, None, 'section', ('expert', 'tensor')), may hold values from 0 to 3, all different within a row; in each aligned block of 64 rows (0 to 63, 64 to 127, ..., all dimensions but the last counted through in order) at most 40 rows name the same one
Outputs:
- blocks_out: bfloat16 [2, 4, 512, 2048], P(None, 'section', ('expert', 'tensor'))
The draws below stay inside these ranges and needn't reach their ends.
Inputs may be any that keep to these rules, and one draw needn't show every extreme that they name: `expert_ids`: within each aligned block of 64 rows (the rows of one device for one tick, direction and section) no expert is named by more than 40 rows, a bound that some block reaches; the two ids of a row differ.
All inputs are finite; a program needn't handle non-finite values.
Results may differ from the reference program's by a relative error of at most 0.0065.
Values may be sent and summed in bfloat16 or wider, within the bound.
A program may use at most 128 MiB of HBM per device.

```python
import math
import jax
import jax.numpy as jnp
import numpy as np
from jax import lax

D = 2048
TOP = 2
FF_DEV = 1408
TOK_DEV = 64
TICKS = 2
SECTIONS = 4
EXPERTS = 4
FF = 2816
TOKENS = 512
CAP = 40
N_TENSOR = 2


def draw_tokens(key, part):
    key_entries = jax.random.fold_in(key, 11)
    key_rows = jax.random.fold_in(key, 12)
    key_cols = jax.random.fold_in(key, 13)
    shape = (2, SECTIONS, TOKENS, D)
    entries = jnp.clip(jax.random.normal(key_entries, shape, jnp.float32), -4.0, 4.0)
    row_scale = jnp.exp(jax.random.uniform(key_rows, (2, SECTIONS, TOKENS, 1), jnp.float32, math.log(0.5), math.log(2.0)))
    col_scale = jnp.exp(jax.random.uniform(key_cols, (1, 1, 1, D), jnp.float32, math.log(0.5), math.log(2.0)))
    values = entries * row_scale * col_scale
    return values.astype(jnp.bfloat16)


def level_of(own_key, dims, shards, low, largest):
    def one(position, blocks):
        steps = jax.random.uniform(jax.random.fold_in(jax.random.fold_in(own_key, 6), position), (blocks,), jnp.float32, low / len(shards), largest / len(shards))
        return jnp.repeat(jnp.exp(steps), dims[position] // blocks).reshape((-1,) + (1,) * (len(dims) - position - 1))

    factor_of = one(*shards[0])
    for cut in shards[1:]:
        factor_of = factor_of * one(*cut)
    return factor_of


def routed_block(own_key, own, number, rows, number_of, top, most, slope):
    order = jax.random.permutation(own_key, number_of)
    packed, usual = portions_of(number_of, rows * top, most, slope, True), portions_of(number_of, rows * top, most, slope, False)
    places = jnp.arange(number_of)

    def named(sizes, rotation):
        used = int((sizes > 0).sum())
        fixed = max(1, used // 4)
        moved = fixed + (places - fixed + rotation * (used - fixed)) % max(1, number_of - fixed)
        return jnp.zeros((number_of,), jnp.int32).at[order[jnp.where(places < fixed, places, moved)]].set(jnp.asarray(sizes, jnp.int32))

    sizes = jnp.where(number % 4 == 0, named(packed, number // 4), named(usual, number - number // 4 - 1))
    mixed = jax.random.permutation(jax.random.fold_in(own, 3), number_of)
    giver, receiver = mixed[0:number_of // 2 * 2:2], mixed[1:number_of // 2 * 2:2]
    slack = jnp.minimum(sizes[giver] - 1, most - sizes[receiver]) // 2
    slack = jnp.where((giver == order[0]) | (receiver == order[0]) | (sizes[receiver] == 0), 0, jnp.maximum(slack, 0))
    moved = jax.random.randint(jax.random.fold_in(own, 4), (number_of // 2,), 0, 1 << 20) % (slack + 1)
    sizes = sizes.at[giver].add(-moved).at[receiver].add(moved)
    items = jnp.searchsorted(jnp.cumsum(sizes), jnp.arange(rows * top), side="right").astype(jnp.int32)
    grid = items.reshape(top, rows).T
    grid = grid[jax.random.permutation(jax.random.fold_in(own, 1), rows)]
    rotation = jax.random.randint(jax.random.fold_in(own, 2), (rows, 1), 0, top)
    return jnp.take_along_axis(grid, (jnp.arange(top)[None, :] + rotation) % top, axis=1)


def portions_of(count, total, reach, lean, full):
    weights = [(1 << 20) // math.isqrt(grade ** lean) + 1 for grade in range(1, count + 1)]
    largest = reach if full else min(reach, max(-(-total // count), total * weights[0] // sum(weights)))
    least = 1 if total - largest >= count - 1 else 0
    given, spare = [largest] + [least] * (count - 1), total - largest - least * (count - 1)
    while spare > 0:
        movable = [i for i in range(1, count) if given[i] < largest] or [i for i in range(1, count) if given[i] < reach]
        whole, budget = sum([weights[i] for i in movable]), spare
        for i in movable:
            addition = min(reach - given[i], max(1, budget * weights[i] // whole), spare)
            given[i] = given[i] + addition
            spare = spare - addition
    return np.array(given)


def normal_values(stream_key, extent, scale, bound, cuts=(), kind=jnp.bfloat16):
    values = jax.random.normal(stream_key, extent, jnp.float32) * scale
    if len(cuts) > 0:
        values = level_of(stream_key, extent, cuts, -0.22, 0.18) * values
    return jnp.clip(values, min=-bound, max=bound).astype(kind)


def setup_inputs(seed: int = 0) -> dict:
    arg_keys = jax.random.split(jax.random.key(seed), 7)
    tokens = draw_tokens(jax.random.fold_in(arg_keys[6], 71), 0)
    norm_gain = jnp.clip(1.0 + 0.18 * jax.random.normal(arg_keys[1], (SECTIONS, D), jnp.float32), 0.099609375, 1.8984375).astype(jnp.bfloat16)
    router_weight = normal_values(arg_keys[2], (SECTIONS, D, EXPERTS), D ** -0.5, 0.125, ((0, 4),))
    gate_up = normal_values(arg_keys[3], (SECTIONS, EXPERTS, D, 2 * FF), D ** -0.5, 0.125, ((0, 4), (1, 4), (3, 2)))
    down_proj = normal_values(arg_keys[4], (SECTIONS, EXPERTS, FF, D), FF ** -0.5, 0.109375, ((0, 4), (1, 4), (2, 2)))
    expert_ids_keys = jax.random.split(jax.random.fold_in(arg_keys[5], 1), TICKS * 2 * SECTIONS * TOKENS // TOK_DEV)
    expert_ids_turns = jax.random.permutation(jax.random.fold_in(arg_keys[5], 3), TICKS * 2 * SECTIONS * TOKENS // TOK_DEV)
    expert_ids = jax.vmap(lambda own, number: routed_block(jax.random.fold_in(arg_keys[5], 2), own, number, TOK_DEV, EXPERTS, TOP, CAP, 2))(expert_ids_keys, expert_ids_turns).reshape((TICKS, 2, SECTIONS, TOKENS, TOP))
    return {"tokens": tokens, "norm_gain": norm_gain, "router_weight": router_weight, "gate_up": gate_up, "down_proj": down_proj, "expert_ids": expert_ids}


EPSILON = 1e-05

def slot_positions(expert_ids, experts, capacity):
    leading, row_count, picked = expert_ids.shape
    flat_ids = expert_ids.reshape(leading, row_count * picked)
    onehot = (flat_ids[:, :, None] == jnp.arange(experts, dtype=jnp.int32)[None, None, :]).astype(jnp.int32)
    running = jnp.cumsum(onehot, axis=1) - 1
    slot_index = lax.optimization_barrier(jnp.sum(running * onehot, axis=2)).astype(jnp.int32)
    return (flat_ids * capacity + slot_index).astype(jnp.int32).reshape(leading, row_count, picked)

def prepare(blocks, gain_row, router, expert_ids, experts, capacity):
    leading, row_count, width = blocks.shape
    values = blocks.astype(jnp.float32)
    scale = lax.rsqrt(lax.optimization_barrier(jnp.mean(values * values, axis=-1, keepdims=True)) + EPSILON)
    normed = (values * scale * gain_row.astype(jnp.float32)).astype(jnp.bfloat16)
    logits = jnp.dot(normed.reshape(-1, width), router, preferred_element_type=jnp.float32)
    logits = logits.reshape(leading, row_count, experts)
    selector = expert_ids[..., None] == jnp.arange(experts, dtype=jnp.int32)
    chosen = lax.optimization_barrier(jnp.sum(jnp.where(selector, logits[:, :, None, :], jnp.float32(0.0)), axis=-1))
    first = jax.nn.sigmoid(chosen[..., 0] - chosen[..., 1])
    second = jax.nn.sigmoid(chosen[..., 1] - chosen[..., 0])
    weights = jnp.stack([first, second], axis=-1)
    positions = slot_positions(expert_ids, experts, capacity)
    table = positions[:, None, :, :] == jnp.arange(experts * capacity, dtype=jnp.int32)[None, :, None, None]
    dispatch = lax.optimization_barrier(jnp.sum(table.astype(jnp.float32), axis=-1))
    routed = jnp.einsum('bpr,brd->bpd', dispatch, normed.astype(jnp.float32)).astype(jnp.bfloat16)
    return (weights, positions, routed)

def combine(blocks, results, weights, positions):
    leading, row_count, width = blocks.shape
    picked = jax.vmap(lambda table_rows, index: table_rows[index])(results, positions.reshape(leading, -1))
    picked = picked.reshape(leading, row_count, 2, width).astype(jnp.float32)
    total = blocks.astype(jnp.float32) + lax.optimization_barrier(jnp.sum(weights[..., None] * picked, axis=2))
    return total.astype(jnp.bfloat16)

def layer(block_rows, gain_row, router, combined_all, down_all, ids):
    blocks_count = TOKENS // TOK_DEV
    grouped = block_rows.reshape(blocks_count, TOK_DEV, D)
    ids_grouped = ids.reshape(blocks_count, TOK_DEV, TOP)
    weights, positions, routed = prepare(grouped, gain_row, router, ids_grouped, EXPERTS, CAP)
    routed = routed.reshape(blocks_count, EXPERTS, CAP, D)

    def one_expert(operands):
        rows_in, combined, down = operands
        flat = rows_in.reshape(-1, D)
        gate_part = jnp.dot(flat, combined[:, :FF], preferred_element_type=jnp.float32).astype(jnp.bfloat16)
        up_part = jnp.dot(flat, combined[:, FF:], preferred_element_type=jnp.float32).astype(jnp.bfloat16)
        gate_part, up_part = lax.optimization_barrier((gate_part, up_part))
        hidden = (jax.nn.silu(gate_part.astype(jnp.float32)) * up_part.astype(jnp.float32)).astype(jnp.bfloat16)
        total = jnp.zeros((flat.shape[0], D), jnp.float32)
        for half_index in range(N_TENSOR):
            start = half_index * FF_DEV
            piece = jnp.dot(hidden[:, start:start + FF_DEV], down[start:start + FF_DEV], preferred_element_type=jnp.float32)
            piece = lax.optimization_barrier(piece.astype(jnp.bfloat16))
            total = total + piece.astype(jnp.float32)
        result = lax.optimization_barrier(total.astype(jnp.bfloat16))
        return result.reshape(blocks_count, CAP, D)
    results = lax.map(one_expert, (jnp.moveaxis(routed, 1, 0), combined_all, down_all))
    results = jnp.moveaxis(results, 0, 1).reshape(blocks_count, EXPERTS * CAP, D)
    return combine(grouped, results, weights, positions).reshape(TOKENS, D)

def reference(tokens, norm_gain, router_weight, gate_up, down_proj, expert_ids):
    state = tokens
    for tick_index in range(TICKS):
        outputs = []
        for direction in range(2):
            per_section = []
            for section_index in range(SECTIONS):
                per_section.append(layer(state[direction, section_index], norm_gain[section_index], router_weight[section_index], gate_up[section_index], down_proj[section_index], expert_ids[tick_index, direction, section_index]))
            outputs.append(jnp.stack(per_section))
        forward = jnp.roll(outputs[0], 1, axis=0)
        backward = jnp.roll(outputs[1], -1, axis=0)
        state = jnp.stack([forward, backward])
    return state
```

```python
import jax
import jax.numpy as jnp
from jax import lax
from jax.sharding import PartitionSpec as P

TOP = 2
TICKS = 2
EPSILON = 1e-05


def shifted(array, axis, by):
    peers = lax.axis_size(axis)
    return lax.ppermute(array, axis, [(i, (i + by) % peers) for i in range(peers)])


def swapped(array):
    halves = lax.axis_size("tensor")
    return lax.ppermute(array, "tensor", [(i, halves - 1 - i) for i in range(halves)])


def passed_on(array, by, cross):
    sections = lax.axis_size("section")
    halves = lax.axis_size("tensor")
    pairs = []
    for s in range(sections):
        for t in range(halves):
            to = halves - 1 - t if cross else t
            pairs.append((s * halves + t, (s + by) % sections * halves + to))
    return lax.ppermute(array, ("section", "tensor"), pairs)


def exchanged(rows, sign):
    experts = lax.axis_size("expert")
    size = rows.shape[0] // experts
    chunks = [rows[d * size : (d + 1) * size] for d in range(experts)]
    if experts != 4:
        got = [chunks[0]] + [shifted(chunks[d], "expert", sign * d) for d in range(1, experts)]
        return jnp.concatenate(got, axis=0)
    half = size // 2
    up = shifted(rows[size : 2 * size + half], "expert", sign)
    down = shifted(rows[2 * size + half :], "expert", -sign)
    up_far = shifted(up[size:], "expert", sign)
    down_far = shifted(down[: size - half], "expert", -sign)
    return jnp.concatenate([chunks[0], up[:size], up_far, down_far, down[size - half :]], axis=0)


def slot_positions(ids, own, experts, capacity):
    blocks, row_count, picked = ids.shape
    flat = ids.reshape(blocks, row_count * picked)
    onehot = (flat[:, :, None] == jnp.arange(experts, dtype=jnp.int32)).astype(jnp.int32)
    running = jnp.cumsum(onehot, axis=1) - 1
    slot = jnp.sum(running * onehot, axis=2)
    away = lax.rem(flat - own + experts, experts)
    block = jnp.arange(blocks, dtype=jnp.int32)[:, None]
    return ((away * blocks + block) * capacity + slot).reshape(blocks * row_count, picked)


def prepare(blocks, gain_row, router, ids, positions, slots):
    values = blocks.astype(jnp.float32)
    scale = lax.rsqrt(jnp.mean(values * values, axis=-1, keepdims=True) + EPSILON)
    normed = (values * scale * gain_row.astype(jnp.float32)).astype(jnp.bfloat16)
    places = jnp.arange(slots, dtype=jnp.int32)
    table = positions[None, :, :] == places[:, None, None]
    dispatch = (table[:, :, 0] | table[:, :, 1]).astype(jnp.bfloat16)
    routed = jnp.dot(dispatch, normed, preferred_element_type=jnp.float32).astype(jnp.bfloat16)
    logits = jnp.dot(normed, router, preferred_element_type=jnp.float32)
    selector = ids[..., None] == jnp.arange(router.shape[1], dtype=jnp.int32)
    chosen = jnp.sum(jnp.where(selector, logits[:, None, :], jnp.float32(0.0)), axis=-1)
    first = jax.nn.sigmoid(chosen[:, 0] - chosen[:, 1])
    second = jax.nn.sigmoid(chosen[:, 1] - chosen[:, 0])
    mixing = jnp.where(positions[:, 0:1] == places, first[:, None], jnp.float32(0.0)) + jnp.where(
        positions[:, 1:2] == places, second[:, None], jnp.float32(0.0)
    )
    return routed, mixing.astype(jnp.bfloat16)


def on_device(tokens, norm_gain, router_weight, gate_up, down_proj, expert_ids):
    experts = lax.axis_size("expert")
    halves = lax.axis_size("tensor")
    row_count = tokens.shape[2]
    capacity = row_count * TOP * 5 // (4 * experts)
    slots = experts * halves * capacity
    first_half = lax.axis_index("tensor") == 0
    own = lax.axis_index("expert")
    combined = gate_up[0, 0]
    units = combined.shape[1] // 2
    down_rows = down_proj[0, 0]
    gain_row = norm_gain[0]
    router = router_weight[0]

    def paired(mine, theirs, axis):
        low = jnp.where(first_half, mine, theirs)
        high = jnp.where(first_half, theirs, mine)
        return jnp.concatenate([low, high], axis=axis)

    ids_own = expert_ids[:, :, 0]
    ids_pair = paired(ids_own, swapped(ids_own), 2)
    state = [paired(tokens[m, 0], swapped(tokens[m, 0]), 0) for m in range(2)]
    for tick in range(TICKS):
        following = []
        for m in range(2):
            by = 1 if m == 0 else -1
            blocks = state[m]
            ids = ids_pair[tick, m]
            positions = slot_positions(
                ids.reshape(halves, row_count, TOP), own, experts, capacity
            )
            routed, mixing = prepare(blocks, gain_row, router, ids, positions, slots)
            expert_rows = exchanged(routed, 1)
            product = jnp.dot(
                expert_rows, combined, preferred_element_type=jnp.float32
            ).astype(jnp.bfloat16)
            low, high = product[:, :units], product[:, units:]
            theirs = swapped(jnp.where(first_half, high, low))
            mine = jnp.where(first_half, low, high)
            gate = jnp.where(first_half, mine, theirs).astype(jnp.float32)
            up = jnp.where(first_half, theirs, mine).astype(jnp.float32)
            hidden = (jax.nn.silu(gate) * up).astype(jnp.bfloat16)
            partial_value = jnp.dot(hidden, down_rows, preferred_element_type=jnp.float32)
            results = exchanged(partial_value.astype(jnp.bfloat16), -1)
            part = jnp.dot(mixing, results, preferred_element_type=jnp.float32)
            kept = blocks.astype(jnp.float32) + part
            if tick == TICKS - 1:
                kept = jnp.where(first_half, kept[:row_count], kept[row_count:])
                part = jnp.where(first_half, part[row_count:], part[:row_count])
            straight = passed_on(kept.astype(jnp.bfloat16), by, False)
            across = passed_on(part.astype(jnp.bfloat16), by, True)
            total = straight.astype(jnp.float32) + across.astype(jnp.float32)
            following.append(total.astype(jnp.bfloat16))
        state = following
    return jnp.stack(state)[:, None]


def solution(mesh):
    in_specs = (
        P(None, "section", ("expert", "tensor"), None),
        P("section", None),
        P("section", None, None),
        P("section", "expert", None, "tensor"),
        P("section", "expert", "tensor", None),
        P(None, None, "section", ("expert", "tensor"), None),
    )
    out_specs = P(None, "section", ("expert", "tensor"), None)
    return jax.shard_map(
        on_device, mesh=mesh, in_specs=in_specs, out_specs=out_specs, check_vma=False
    )
```
